256 devices in a mesh: parts: 4 (over x, y), pts: 64 (over z, core).
Axes of the slice: x: 2, y: 2, z: 32, core: 2. Of those that a mesh axis runs over, the one named last changes fastest.
The devices are a block of a 4x8x32 slice.
Arguments:
- grid_weights: float32 [512, 128, 128], P(('parts', 'pts')), parts along dimension 0, may hold values from -6 to 6
- direction: float32 [512, 128, 128], P(('parts', 'pts')), parts along dimension 0, may hold values from -6 to 6
- kern_x: float32 [128, 128], replicated
- kern_y: float32 [128, 128], replicated
- kern_z: float32 [128, 128], replicated
- interp: bfloat16 [32768, 128, 256], P(('parts', 'pts')), parts along dimension 0, may hold values from -4 to 4
- block_corner: int32 [3, 32768], P(None, ('parts', 'pts')), parts along dimension 1, may hold values from 0 to 120, as said below
- block_offsets: int32 [32768, 256], P(('parts', 'pts')), parts along dimension 0, may hold values from 0 to 2047, as said below
- labels: int32 [32768, 128], P(('parts', 'pts')), parts along dimension 0, may hold values 0 or 1
- trial_steps: float32 [5], replicated, may hold values from 0.05 to 2
- accept: int32 [1], replicated, may hold values from 0 to 4
Outputs:
- new_weights: float32 [512, 128, 128], P(('parts', 'pts')), parts along dimension 0
- grid_gradient: float32 [512, 128, 128], P(('parts', 'pts')), parts along dimension 0
- curvature: float32 [32768, 128], P(('parts', 'pts')), parts along dimension 0
- trial_objective: float32 [20], P('parts'), parts along dimension 0
- trial_slope: float32 [20], P('parts'), parts along dimension 0
The draws below stay inside these ranges and needn't reach their ends.
There are 4 independent parts, one for each index of `parts`. The reference program is written for one: setup_inputs(seed, part) draws one part's arguments, and reference() takes and returns one part's arrays. A program takes and returns all parts, laid end to end along the dimension named above; an argument that names none is the same for every part. Nothing has to cross between parts.
Inputs may be any that keep to these rules, and one draw needn't show every extreme that they name: `block_corner`: row 0 lies in 0 to 112, row 1 in 0 to 112, row 2 in 0 to 120. `block_offsets`: the 256 offsets of one block are distinct.
All inputs are finite; a program needn't handle non-finite values. No bound on the sum of `labels` on one device may be relied on, other than what follows from the above.
Results may differ from the reference program's by a relative error of at most 0.0075.
The reference program's roundings to bfloat16 on the way count: a program that leaves them out, or rounds other values in their place, can miss the bound.
Values may be sent and summed in bfloat16 or wider, within the bound.
A program may use at most 128 MiB of HBM per device.

```python
import math
import jax
import jax.numpy as jnp
from jax import lax

GX = 128
GY = 128
GZ = 128
BOXX = 16
BOXY = 16
BOXZ = 8
COLS = 256
PTS_BLOCK = 128
NTRIAL = 5
NB = 128
BLOCKS = 8192
POINTS = 1048576
N_PTS = 64


def kernel_table(key, size, salt):
    key = jax.random.fold_in(key, salt)
    key_len, key_noise, key_gain = jax.random.split(key, 3)
    length = jax.random.uniform(key_len, (), jnp.float32, 4.0, 16.0)
    noise_scale = 0.15
    position = jnp.arange(size, dtype=jnp.float32)
    spacing = jnp.abs(position[:, None] - position[None, :])
    smooth = jnp.exp(-spacing / length)
    noise = jax.random.normal(key_noise, (size, size), jnp.float32)
    symmetric = (noise + noise.T) * 0.7071
    gains = jax.random.uniform(key_gain, (size,), jnp.float32, 0.7, 1.4)
    table = gains[:, None] * (smooth + noise_scale * symmetric) * gains[None, :] / jnp.sqrt(length)
    return table.astype(jnp.float32)


def draw_kern_x(key, part):
    return kernel_table(key, GX, 11)


def draw_kern_y(key, part):
    return kernel_table(key, GY, 23)


def draw_kern_z(key, part):
    return kernel_table(key, GZ, 37)


def draw_interp(key, part):
    key = jax.random.fold_in(key, 53)
    ratio = 6.0
    base = jnp.clip(jax.random.normal(key, (BLOCKS, PTS_BLOCK, COLS), jnp.float32), -4.0, 4.0)
    level = jnp.arange(BLOCKS, dtype=jnp.float32) / max(BLOCKS - 1, 1)
    scale = jnp.exp(jnp.log(ratio) * level) / jnp.sqrt(ratio)
    table = base * scale[:, None, None] / jnp.sqrt(jnp.float32(COLS))
    return jnp.clip(table, -4.0, 4.0).astype(jnp.bfloat16)


def draw_block_corner(key, part):
    limits = jnp.array([GX - BOXX, GY - BOXY, GZ - BOXZ], jnp.int32)
    corner = jax.random.randint(key, (3, BLOCKS), 0, limits[:, None] + 1)
    corner = corner.at[:, 0].set(limits)
    corner = corner.at[:, BLOCKS - 1].set(0)
    return corner.astype(jnp.int32)


def draw_block_offsets(key, part):
    keys = jax.random.split(key, BLOCKS)

    def choose_cells(one_key):
        return jax.random.permutation(one_key, BOXX * BOXY * BOXZ)[:COLS]
    return jax.vmap(choose_cells)(keys).astype(jnp.int32)


def place_ends(values, rng, smallest, top_value):
    longest = values.shape.index(max(values.shape))
    spots = []
    for shift in (0, 1):
        where = [jax.random.randint(jax.random.fold_in(rng, axis), (), 0, length) for axis, length in enumerate(values.shape)]
        where[longest] = (where[longest] + shift) % values.shape[longest]
        spots.append(tuple(where))
    return values.at[spots[0]].set(smallest).at[spots[1]].set(top_value)


def levels(rng, shape, pieces, smallest, top_value):
    def one(dim, blocks):
        steps = jax.random.uniform(jax.random.fold_in(jax.random.fold_in(rng, 6), dim), (blocks,), jnp.float32, smallest / len(pieces), top_value / len(pieces))
        return jnp.repeat(jnp.exp(steps), shape[dim] // blocks).reshape((-1,) + (1,) * (len(shape) - dim - 1))

    level = one(*pieces[0])
    for cut in pieces[1:]:
        level = level * one(*cut)
    return level


def bell_draw(rng, dims, width, limit, shards=(), held_as=jnp.bfloat16):
    values = width * jax.random.normal(rng, dims, jnp.float32)
    if shards:
        values = values * levels(rng, dims, shards, -0.22, 0.18)
    return jnp.clip(values, -limit, limit).astype(held_as)


def setup_inputs(seed: int = 0, part: int = 0) -> dict:
    key_list = jax.random.split(jax.random.key(seed), 12)
    own_keys = jax.random.split(jax.random.fold_in(key_list[11], part), 12)
    grid_weights = bell_draw(own_keys[0], (GX, GY, GZ), 1.0, 6.0, ((0, 64),), jnp.float32)
    direction = bell_draw(own_keys[1], (GX, GY, GZ), 1.0, 6.0, ((0, 64),), jnp.float32)
    kern_x = draw_kern_x(jax.random.fold_in(key_list[11], 71), part)
    kern_y = draw_kern_y(jax.random.fold_in(key_list[11], 71), part)
    kern_z = draw_kern_z(jax.random.fold_in(key_list[11], 71), part)
    interp = draw_interp(jax.random.fold_in(jax.random.fold_in(key_list[11], part), 71), part)
    block_corner = draw_block_corner(jax.random.fold_in(jax.random.fold_in(key_list[11], part), 71), part)
    block_offsets = draw_block_offsets(jax.random.fold_in(jax.random.fold_in(key_list[11], part), 71), part)
    labels = place_ends((jax.random.randint(own_keys[8], (BLOCKS, PTS_BLOCK), 0, 2) < 1).astype(jnp.int32), jax.random.fold_in(own_keys[8], 1), 0, 1)
    trial_steps = jnp.clip(jnp.exp(jax.random.uniform(key_list[9], (NTRIAL,), jnp.float32, math.log(0.05), math.log(2.0))), 0.05, 2.0)
    accept = jax.random.randint(key_list[10], (1,), 0, NTRIAL).astype(jnp.int32)
    return dict(grid_weights=grid_weights, direction=direction, kern_x=kern_x, kern_y=kern_y, kern_z=kern_z, interp=interp, block_corner=block_corner, block_offsets=block_offsets, labels=labels, trial_steps=trial_steps, accept=accept)


HIGHEST = lax.Precision.HIGHEST


def plane_mix(fields, kern_y, kern_z):
    inner_mix = jnp.einsum('...bc,zc->...bz', fields, kern_z, precision=HIGHEST)
    return jnp.einsum('...xbz,yb->...xyz', inner_mix, kern_y, precision=HIGHEST).astype(jnp.bfloat16)


def depth_mix(partial_value, kern_x):
    return jnp.einsum('xa,...ayz->...xyz', kern_x, partial_value.astype(jnp.float32), precision=HIGHEST)


def cell_ids_of(block_corner, block_offsets):
    plane_off = block_offsets // (BOXY * BOXZ)
    row_off = (block_offsets // BOXZ) % BOXY
    depth_off = block_offsets % BOXZ
    cell_x = block_corner[0][:, None] + plane_off
    cell_y = block_corner[1][:, None] + row_off
    cell_z = block_corner[2][:, None] + depth_off
    return ((cell_x * GY + cell_y) * GZ + cell_z).astype(jnp.int32)


def interpolate(interp, values):
    count_fields = values.shape[0]
    groups = interp.reshape(N_PTS, NB, PTS_BLOCK, COLS)
    grouped = jnp.moveaxis(values.reshape(count_fields, N_PTS, NB, COLS), 1, 0)

    def one_group(operands):
        return jnp.einsum('bpc,fbc->fbp', operands[0].astype(jnp.float32), operands[1].astype(jnp.float32), precision=HIGHEST)

    result = lax.map(one_group, (groups, grouped))
    return jnp.moveaxis(result, 0, 1).reshape(count_fields, N_PTS * NB, PTS_BLOCK)


def column_terms(interp, residual):
    groups = interp.reshape(N_PTS, NB, PTS_BLOCK, COLS)
    grouped = residual.reshape(N_PTS, NB, PTS_BLOCK)

    def one_group(operands):
        return jnp.einsum('bpc,bp->bc', operands[0].astype(jnp.float32), operands[1].astype(jnp.float32), precision=HIGHEST)

    return lax.map(one_group, (groups, grouped)).reshape(N_PTS * NB, COLS)


def reference(grid_weights, direction, kern_x, kern_y, kern_z, interp, block_corner, block_offsets, labels, trial_steps, accept):
    fields = jnp.stack([grid_weights, direction])
    mixed_grid = depth_mix(plane_mix(fields, kern_y, kern_z), kern_x)
    quad_gu = jnp.sum(grid_weights * mixed_grid[0])
    quad_du = jnp.sum(direction * mixed_grid[0])
    quad_dv = jnp.sum(direction * mixed_grid[1])
    cell_ids = cell_ids_of(block_corner, block_offsets)
    flat_grid = mixed_grid.astype(jnp.bfloat16).reshape(2, -1)
    values = jnp.take(flat_grid, cell_ids, axis=1)
    latent_pair = interpolate(interp, values)
    latent = latent_pair[0]
    slope_pt = latent_pair[1]
    target = labels.astype(jnp.float32)
    signed = 2.0 * target - 1.0
    trial_latent = latent[None] + trial_steps[:, None, None] * slope_pt[None]
    loglik = jnp.sum(jax.nn.log_sigmoid(signed[None] * trial_latent), axis=(1, 2))
    descent = jnp.sum((target[None] - jax.nn.sigmoid(trial_latent)) * slope_pt[None], axis=(1, 2))
    prior = 0.5 * (quad_gu + 2.0 * trial_steps * quad_du + trial_steps * trial_steps * quad_dv)
    trial_objective = (loglik - prior) / POINTS
    trial_slope = (descent - quad_du - trial_steps * quad_dv) / POINTS
    chosen = jnp.sum(jnp.where(jnp.arange(NTRIAL) == accept[0], trial_steps, 0.0))
    probability = jax.nn.sigmoid(latent + chosen * slope_pt)
    residual = (target - probability).astype(jnp.bfloat16)
    column_term = column_terms(interp, residual)
    spread = jnp.zeros((GX * GY * GZ,), jnp.float32).at[cell_ids.reshape(-1)].add(column_term.reshape(-1)).reshape(GX, GY, GZ)
    new_weights = grid_weights + chosen * direction
    grid_gradient = spread - new_weights
    bend_grid = depth_mix(plane_mix(grid_gradient[None], kern_y, kern_z), kern_x)
    bend_values = jnp.take(bend_grid.astype(jnp.bfloat16).reshape(1, -1), cell_ids, axis=1)
    bend_pt = interpolate(interp, bend_values)[0]
    curvature = probability * (1.0 - probability) * bend_pt
    return new_weights, grid_gradient, curvature, trial_objective, trial_slope
```

```python
import functools

import jax
import jax.numpy as jnp
from jax import lax
from jax.experimental import pallas as pl
from jax.experimental.pallas import tpu as pltpu
from jax.sharding import Mesh
from jax.sharding import PartitionSpec as P

BOXX = 16
BOXY = 16
BOXZ = 8
NTRIAL = 5
PTS = ("pts_0", "pts_1")
PARTS_PTS = ("parts", "pts_0", "pts_1")
HIGHEST = lax.Precision.HIGHEST
F32 = jnp.float32
BF16 = jnp.bfloat16
LINE = 136
ZC = 16
XW = 32
VMEM_CAP = 60 * 1024 * 1024
NT = (((1,), (1,)), ((), ()))


def depth_mix(fields, gath_ref, kxs_ref, lines, img_ref, on_rows):
    depth = img_ref.shape[1]
    count_a = gath_ref.shape[0]

    def chunk(k, carry):
        z0 = pl.multiple_of(k * ZC, ZC)

        def place(i, c):
            for u in range(8):
                a = i * 8 + u
                for f in range(fields):
                    lines[f][pl.ds(a, ZC, stride=LINE), :] = gath_ref[a, f, pl.ds(z0, ZC), :].astype(F32)
            return c

        lax.fori_loop(0, count_a // 8, place, 0)
        for zi in range(ZC):
            rows = [lines[f][zi * LINE : zi * LINE + count_a, :].astype(BF16) for f in range(fields)]
            wide = rows[0] if fields == 1 else jnp.concatenate(rows, axis=1)
            mixed = jnp.dot(kxs_ref[...], jnp.concatenate([wide, wide], axis=0), preferred_element_type=F32)
            for f in range(fields):
                img_ref[f, z0 + zi] = mixed[:count_a, f * 128 : (f + 1) * 128].astype(BF16)
            if on_rows is not None:
                carry = on_rows(z0 + zi, mixed[count_a : count_a + 8, :], carry)
        return carry

    zero = jnp.zeros((8, 128), F32)
    return lax.fori_loop(0, depth // ZC, chunk, (zero, zero))


def box_of(b, corner_ref, offs_ref):
    cx = corner_ref[0, b]
    cy = corner_ref[1, b]
    cz = corner_ref[2, b]
    x0 = pl.multiple_of(jnp.minimum((cx // 16) * 16, 128 - XW), 16)
    off = offs_ref[pl.ds(b, 1), :]
    row = (off & (BOXZ - 1)) * XW + (off >> 7) + (cx - x0)
    line = ((off >> 3) & (BOXY - 1)) + cy
    return x0, cz, row, line


def pick(fields, b, corner_ref, offs_ref, img_ref, iota_y, iota_r):
    x0, cz, row, line = box_of(b, corner_ref, offs_ref)
    boxes = [img_ref[f, pl.ds(cz, BOXZ), pl.ds(x0, XW), :].reshape(BOXZ * XW, 128) for f in range(fields)]
    box = boxes[0] if fields == 1 else jnp.concatenate(boxes, axis=0)
    onehot = jnp.where(iota_y == line, 1.0, 0.0).astype(BF16)
    lanes = jnp.dot(box, onehot, preferred_element_type=F32)
    wanted = iota_r == row
    n = BOXZ * XW
    return [
        jnp.sum(jnp.where(wanted, lanes[f * n : (f + 1) * n], 0.0), axis=0, keepdims=True)
        for f in range(fields)
    ]


def points_kernel(
    corner_ref,
    steps_ref,
    accept_ref,
    gath_ref,
    kxs_ref,
    own_ref,
    offs_ref,
    interp_ref,
    labels_ref,
    stats_ref,
    bend_scale_ref,
    spread_ref,
    line_u,
    line_v,
    img_ref,
    lat_ref,
    slope_ref,
    res_ref,
    acc_ref,
):
    blocks, _, cols = interp_ref.shape

    def on_rows(z, mixed, carry):
        own = own_ref[z]
        return (carry[0] + mixed[:, :128] * own, carry[1] + mixed[:, 128:] * own)

    quad_u, quad_v = depth_mix(2, gath_ref, kxs_ref, (line_u, line_v), img_ref, on_rows)
    iota_y = lax.broadcasted_iota(jnp.int32, (128, cols), 0)
    iota_r = lax.broadcasted_iota(jnp.int32, (BOXZ * XW, cols), 0)
    iota_8 = lax.broadcasted_iota(jnp.int32, (16, cols), 0)

    def gather_step(i, c):
        for u in range(UNROLL):
            b = i * UNROLL + u
            first, second = pick(2, b, corner_ref, offs_ref, img_ref, iota_y, iota_r)
            pair = jnp.where(iota_8 == 0, first, jnp.where(iota_8 == 1, second, 0.0)).astype(BF16)
            both = lax.dot_general(pair, interp_ref[b], NT, preferred_element_type=F32)
            lat_ref[pl.ds(b, 1), :] = both[0:1]
            slope_ref[pl.ds(b, 1), :] = both[1:2]
        return c

    lax.fori_loop(0, blocks // UNROLL, gather_step, 0)

    lat = lat_ref[...]
    slope = slope_ref[...]
    target = labels_ref[...].astype(F32)
    signed = 2.0 * target - 1.0
    stats_ref[...] = jnp.zeros_like(stats_ref)
    chosen = steps_ref[0]
    for k in range(1, NTRIAL):
        chosen = jnp.where(accept_ref[0] == k, steps_ref[k], chosen)
    for k in range(NTRIAL):
        q = lat + steps_ref[k] * slope
        s = signed * q
        loglik = jnp.minimum(s, 0.0) - jnp.log1p(jnp.exp(-jnp.abs(s)))
        stats_ref[k : k + 1, :] = jnp.sum(loglik, axis=0, keepdims=True)
        descent = (target - jax.nn.sigmoid(q)) * slope
        stats_ref[NTRIAL + k : NTRIAL + k + 1, :] = jnp.sum(descent, axis=0, keepdims=True)
    stats_ref[10:11, :] = quad_u[0:1] + quad_u[1:2]
    stats_ref[11:12, :] = quad_u[2:3] + quad_u[3:4]
    stats_ref[12:13, :] = quad_v[2:3] + quad_v[3:4]
    prob = jax.nn.sigmoid(lat + chosen * slope)
    bend_scale_ref[...] = prob * (1.0 - prob)
    res_ref[...] = (target - prob).astype(BF16).astype(F32)

    def clear(i, c):
        acc_ref[pl.ds(pl.multiple_of(i * LINE, 8), LINE), :] = jnp.zeros((LINE, 128), F32)
        return c

    lax.fori_loop(0, spread_ref.shape[1], clear, 0)

    def scatter_step(i, c):
        for u in range(UNROLL):
            b = i * UNROLL + u
            x0, cz, row, line = box_of(b, corner_ref, offs_ref)
            res = jnp.broadcast_to(res_ref[pl.ds(b, 1), :], (16, 128)).astype(BF16)
            term = jnp.dot(res, interp_ref[b], preferred_element_type=F32)[0:1]
            high = term.astype(BF16).astype(F32)
            low = term - high
            at_y = iota_y == line
            placed = jnp.concatenate([jnp.where(at_y, high, 0.0), jnp.where(at_y, low, 0.0)], axis=0).astype(BF16)
            onehot = jnp.where(iota_r == row, 1.0, 0.0).astype(BF16)
            both = lax.dot_general(onehot, placed, NT, preferred_element_type=F32)
            box = both[:, :128] + both[:, 128:]
            for d in range(BOXZ):
                at = pl.ds(pl.multiple_of((cz + d) * LINE + x0, 8), XW)
                acc_ref[at, :] = acc_ref[at, :] + box[d * XW : (d + 1) * XW]
        return c

    lax.fori_loop(0, blocks // UNROLL, scatter_step, 0)

    def emit(i, c):
        for u in range(4):
            x = i * 4 + u
            spread_ref[x] = acc_ref[pl.ds(x, spread_ref.shape[1], stride=LINE), :].astype(BF16)
        return c

    lax.fori_loop(0, spread_ref.shape[0] // 4, emit, 0)


UNROLL = 4


def bend_kernel(corner_ref, gath_ref, kxs_ref, offs_ref, interp_ref, scale_ref, curv_ref, line_u, img_ref):
    blocks, _, cols = interp_ref.shape
    depth_mix(1, gath_ref, kxs_ref, (line_u,), img_ref, None)
    iota_y = lax.broadcasted_iota(jnp.int32, (128, cols), 0)
    iota_r = lax.broadcasted_iota(jnp.int32, (BOXZ * XW, cols), 0)

    def step(i, c):
        for u in range(UNROLL):
            b = i * UNROLL + u
            (value,) = pick(1, b, corner_ref, offs_ref, img_ref, iota_y, iota_r)
            rows = jnp.broadcast_to(value, (16, cols)).astype(BF16)
            bend = lax.dot_general(rows, interp_ref[b], NT, preferred_element_type=F32)
            curv_ref[pl.ds(b, 1), :] = scale_ref[pl.ds(b, 1), :] * bend[0:1]
        return c

    lax.fori_loop(0, blocks // UNROLL, step, 0)


VM = pl.BlockSpec(memory_space=pltpu.VMEM)
SM = pl.BlockSpec(memory_space=pltpu.SMEM)


def split(values, count):
    terms = []
    for _ in range(count):
        high = lax.reduce_precision(values, 8, 7)
        terms.append(high.astype(BF16))
        values = values - high
    return terms


def split_pair(table):
    return jnp.concatenate(split(table, 2), axis=1)


def plane_of(fields, kern_y, kern_z):
    inner = jnp.einsum("fxbc,zc->fxbz", fields, kern_z, precision=HIGHEST)
    return jnp.einsum("fxbz,yb->xfzy", inner, kern_y, precision=HIGHEST).astype(BF16)


def body(
    grid_weights,
    direction,
    kern_x,
    kern_y,
    kern_z,
    interp,
    block_corner,
    block_offsets,
    labels,
    trial_steps,
    accept,
):
    slab, size_y, size_z = grid_weights.shape
    devices = lax.axis_size(PTS)
    size_x = slab * devices
    blocks, per_block, cols = interp.shape
    points = blocks * per_block * devices
    me = lax.axis_index(PTS)

    plane = plane_of(jnp.stack([grid_weights, direction]), kern_y, kern_z)
    gathered = lax.all_gather(plane, PTS, axis=0, tiled=True)
    mine = lax.dynamic_slice_in_dim(kern_x, me * slab, slab, 0)
    tall = jnp.concatenate([kern_x, mine, mine, jnp.zeros((16 - 2 * slab, size_x), F32)], axis=0)
    kxs = split_pair(tall)
    own = jnp.concatenate([grid_weights, direction], axis=0).transpose(2, 0, 1)
    own = jnp.pad(own, ((0, 0), (0, 8 - 2 * slab), (0, 0)))
    stats, bend_scale, spread_all = pl.pallas_call(
        points_kernel,
        name="points",
        in_specs=[SM, SM, SM, VM, VM, VM, VM, VM, VM],
        out_specs=[VM, VM, VM],
        out_shape=[
            jax.ShapeDtypeStruct((16, 128), F32),
            jax.ShapeDtypeStruct((blocks, per_block), F32),
            jax.ShapeDtypeStruct((size_x, size_z, size_y), BF16),
        ],
        scratch_shapes=[
            pltpu.VMEM(((ZC + 1) * LINE, 128), F32),
            pltpu.VMEM(((ZC + 1) * LINE, 128), F32),
            pltpu.VMEM((2, size_z, size_x, size_y), BF16),
            pltpu.VMEM((blocks, per_block), F32),
            pltpu.VMEM((blocks, per_block), F32),
            pltpu.VMEM((blocks, per_block), F32),
            pltpu.VMEM(((size_z + 1) * LINE, 128), F32),
        ],
        compiler_params=pltpu.CompilerParams(vmem_limit_bytes=VMEM_CAP),
    )(block_corner, trial_steps, accept, gathered, kxs, own, block_offsets, interp, labels)

    chosen = jnp.sum(jnp.where(jnp.arange(NTRIAL) == accept[0], trial_steps, 0.0))
    new_weights = grid_weights + chosen * direction
    pair = lax.axis_size(PTS[1])
    tiles = spread_all.reshape(devices // pair, pair, slab, size_z, size_y)
    tiles = lax.psum_scatter(jnp.moveaxis(tiles, 1, 0), PTS[1], scatter_dimension=0, tiled=True)[0]
    spread = lax.psum_scatter(tiles, PTS[0], scatter_dimension=0, tiled=True)[0]
    grid_gradient = spread.astype(F32).transpose(0, 2, 1) - new_weights

    bend_plane = plane_of(grid_gradient[None], kern_y, kern_z)
    tail = jnp.pad(jnp.stack(split(jnp.sum(stats, axis=1), 3), axis=1), ((0, 0), (0, size_y - 3)))
    tail = jnp.stack([tail] + [jnp.zeros_like(tail)] * (slab - 1))[:, None]
    bend_gathered = lax.all_gather(jnp.concatenate([bend_plane, tail], axis=2), PTS, axis=0, tiled=True)
    tails = bend_gathered.reshape(devices, slab, size_z + 16, size_y)[:, 0, size_z:, :3]
    sums = jnp.sum(tails.astype(F32), axis=(0, 2))
    loglik = sums[:NTRIAL]
    descent = sums[NTRIAL : 2 * NTRIAL]
    quad_gu, quad_du, quad_dv = sums[10], sums[11], sums[12]
    prior = 0.5 * (quad_gu + 2.0 * trial_steps * quad_du + trial_steps * trial_steps * quad_dv)
    trial_objective = (loglik - prior) / points
    trial_slope = (descent - quad_du - trial_steps * quad_dv) / points

    curvature = pl.pallas_call(
        bend_kernel,
        name="bend",
        in_specs=[SM, VM, VM, VM, VM, VM],
        out_specs=VM,
        out_shape=jax.ShapeDtypeStruct((blocks, per_block), F32),
        scratch_shapes=[
            pltpu.VMEM(((ZC + 1) * LINE, 128), F32),
            pltpu.VMEM((1, size_z, size_x, size_y), BF16),
        ],
        compiler_params=pltpu.CompilerParams(vmem_limit_bytes=VMEM_CAP),
    )(block_corner, bend_gathered, split_pair(kern_x), block_offsets, interp, bend_scale)
    return (new_weights, grid_gradient, curvature, trial_objective, trial_slope)


def solution(mesh):
    cores = 2
    chips = mesh.shape["pts"] // cores
    finer = Mesh(mesh.devices.reshape(mesh.shape["parts"], chips, cores), PARTS_PTS)
    placed = (
        P(PARTS_PTS, None, None),
        P(PARTS_PTS, None, None),
        P(),
        P(),
        P(),
        P(PARTS_PTS, None, None),
        P(None, PARTS_PTS),
        P(PARTS_PTS, None),
        P(PARTS_PTS, None),
        P(),
        P(),
    )
    return jax.shard_map(
        body,
        mesh=finer,
        in_specs=placed,
        out_specs=(
            P(PARTS_PTS, None, None),
            P(PARTS_PTS, None, None),
            P(PARTS_PTS, None),
            P("parts"),
            P("parts"),
        ),
        check_vma=False,
    )
```

```python
import functools

import jax
import jax.numpy as jnp
from jax import lax
from jax.experimental import pallas as pl
from jax.experimental.pallas import tpu as pltpu
from jax.sharding import Mesh
from jax.sharding import PartitionSpec as P

BOXX = 16
BOXY = 16
BOXZ = 8
NTRIAL = 5
PTS = ("pts_0", "pts_1")
PARTS_PTS = ("parts", "pts_0", "pts_1")
HIGHEST = lax.Precision.HIGHEST
F32 = jnp.float32
BF16 = jnp.bfloat16
LINE = 136
ZC = 16
XW = 32
VMEM_CAP = 60 * 1024 * 1024
MESH = pl.DeviceIdType.MESH
NT = (((1,), (1,)), ((), ()))


def depth_mix(fields, gath_ref, kxs_ref, lines, img_ref, on_rows):
    depth = img_ref.shape[1]
    count_a = gath_ref.shape[0]

    def chunk(k, carry):
        z0 = pl.multiple_of(k * ZC, ZC)

        def place(i, c):
            for u in range(8):
                a = i * 8 + u
                for f in range(fields):
                    lines[f][pl.ds(a, ZC, stride=LINE), :] = gath_ref[a, f, pl.ds(z0, ZC), :].astype(F32)
            return c

        lax.fori_loop(0, count_a // 8, place, 0)
        for zi in range(ZC):
            rows = [lines[f][zi * LINE : zi * LINE + count_a, :].astype(BF16) for f in range(fields)]
            wide = rows[0] if fields == 1 else jnp.concatenate(rows, axis=1)
            mixed = jnp.dot(kxs_ref[...], jnp.concatenate([wide, wide], axis=0), preferred_element_type=F32)
            for f in range(fields):
                img_ref[f, z0 + zi] = mixed[:count_a, f * 128 : (f + 1) * 128].astype(BF16)
            if on_rows is not None:
                carry = on_rows(z0 + zi, mixed[count_a : count_a + 8, :], carry)
        return carry

    zero = jnp.zeros((8, 128), F32)
    return lax.fori_loop(0, depth // ZC, chunk, (zero, zero))


def box_of(b, corner_ref, offs_ref):
    cx = corner_ref[0, b]
    cy = corner_ref[1, b]
    cz = corner_ref[2, b]
    x0 = pl.multiple_of(jnp.minimum((cx // 16) * 16, 128 - XW), 16)
    off = offs_ref[pl.ds(b, 1), :]
    row = (off & (BOXZ - 1)) * XW + (off >> 7) + (cx - x0)
    line = ((off >> 3) & (BOXY - 1)) + cy
    return x0, cz, row, line


def pick(fields, b, corner_ref, offs_ref, img_ref, iota_y, iota_r):
    x0, cz, row, line = box_of(b, corner_ref, offs_ref)
    boxes = [img_ref[f, pl.ds(cz, BOXZ), pl.ds(x0, XW), :].reshape(BOXZ * XW, 128) for f in range(fields)]
    box = boxes[0] if fields == 1 else jnp.concatenate(boxes, axis=0)
    onehot = jnp.where(iota_y == line, 1.0, 0.0).astype(BF16)
    lanes = jnp.dot(box, onehot, preferred_element_type=F32)
    wanted = iota_r == row
    n = BOXZ * XW
    return [
        jnp.sum(jnp.where(wanted, lanes[f * n : (f + 1) * n], 0.0), axis=0, keepdims=True)
        for f in range(fields)
    ]


def points_kernel(
    corner_ref,
    steps_ref,
    accept_ref,
    gath_ref,
    kxs_ref,
    own_ref,
    offs_ref,
    interp_ref,
    labels_ref,
    stats_ref,
    bend_scale_ref,
    spread_ref,
    line_u,
    line_v,
    img_ref,
    lat_ref,
    slope_ref,
    res_ref,
    acc_ref,
):
    blocks, _, cols = interp_ref.shape

    def on_rows(z, mixed, carry):
        own = own_ref[z]
        return (carry[0] + mixed[:, :128] * own, carry[1] + mixed[:, 128:] * own)

    quad_u, quad_v = depth_mix(2, gath_ref, kxs_ref, (line_u, line_v), img_ref, on_rows)
    iota_y = lax.broadcasted_iota(jnp.int32, (128, cols), 0)
    iota_r = lax.broadcasted_iota(jnp.int32, (BOXZ * XW, cols), 0)
    iota_8 = lax.broadcasted_iota(jnp.int32, (16, cols), 0)

    def gather_step(i, c):
        for u in range(UNROLL):
            b = i * UNROLL + u
            first, second = pick(2, b, corner_ref, offs_ref, img_ref, iota_y, iota_r)
            pair = jnp.where(iota_8 == 0, first, jnp.where(iota_8 == 1, second, 0.0)).astype(BF16)
            both = lax.dot_general(pair, interp_ref[b], NT, preferred_element_type=F32)
            lat_ref[pl.ds(b, 1), :] = both[0:1]
            slope_ref[pl.ds(b, 1), :] = both[1:2]
        return c

    lax.fori_loop(0, blocks // UNROLL, gather_step, 0)

    lat = lat_ref[...]
    slope = slope_ref[...]
    target = labels_ref[...].astype(F32)
    signed = 2.0 * target - 1.0
    stats_ref[...] = jnp.zeros_like(stats_ref)
    chosen = steps_ref[0]
    for k in range(1, NTRIAL):
        chosen = jnp.where(accept_ref[0] == k, steps_ref[k], chosen)
    for k in range(NTRIAL):
        q = lat + steps_ref[k] * slope
        s = signed * q
        loglik = jnp.minimum(s, 0.0) - jnp.log1p(jnp.exp(-jnp.abs(s)))
        stats_ref[k : k + 1, :] = jnp.sum(loglik, axis=0, keepdims=True)
        descent = (target - jax.nn.sigmoid(q)) * slope
        stats_ref[NTRIAL + k : NTRIAL + k + 1, :] = jnp.sum(descent, axis=0, keepdims=True)
    stats_ref[10:11, :] = quad_u[0:1] + quad_u[1:2]
    stats_ref[11:12, :] = quad_u[2:3] + quad_u[3:4]
    stats_ref[12:13, :] = quad_v[2:3] + quad_v[3:4]
    prob = jax.nn.sigmoid(lat + chosen * slope)
    bend_scale_ref[...] = prob * (1.0 - prob)
    res_ref[...] = (target - prob).astype(BF16).astype(F32)

    def clear(i, c):
        acc_ref[pl.ds(pl.multiple_of(i * LINE, 8), LINE), :] = jnp.zeros((LINE, 128), F32)
        return c

    lax.fori_loop(0, spread_ref.shape[1], clear, 0)

    def scatter_step(i, c):
        for u in range(UNROLL):
            b = i * UNROLL + u
            x0, cz, row, line = box_of(b, corner_ref, offs_ref)
            res = jnp.broadcast_to(res_ref[pl.ds(b, 1), :], (16, 128)).astype(BF16)
            term = jnp.dot(res, interp_ref[b], preferred_element_type=F32)[0:1]
            high = term.astype(BF16).astype(F32)
            low = term - high
            at_y = iota_y == line
            placed = jnp.concatenate([jnp.where(at_y, high, 0.0), jnp.where(at_y, low, 0.0)], axis=0).astype(BF16)
            onehot = jnp.where(iota_r == row, 1.0, 0.0).astype(BF16)
            both = lax.dot_general(onehot, placed, NT, preferred_element_type=F32)
            box = both[:, :128] + both[:, 128:]
            for d in range(BOXZ):
                at = pl.ds(pl.multiple_of((cz + d) * LINE + x0, 8), XW)
                acc_ref[at, :] = acc_ref[at, :] + box[d * XW : (d + 1) * XW]
        return c

    lax.fori_loop(0, blocks // UNROLL, scatter_step, 0)

    def emit(i, c):
        for u in range(4):
            x = i * 4 + u
            spread_ref[x] = acc_ref[pl.ds(x, spread_ref.shape[1], stride=LINE), :].astype(BF16)
        return c

    lax.fori_loop(0, spread_ref.shape[0] // 4, emit, 0)


UNROLL = 4


def bend_kernel(corner_ref, gath_ref, kxs_ref, offs_ref, interp_ref, scale_ref, curv_ref, line_u, img_ref):
    blocks, _, cols = interp_ref.shape
    depth_mix(1, gath_ref, kxs_ref, (line_u,), img_ref, None)
    iota_y = lax.broadcasted_iota(jnp.int32, (128, cols), 0)
    iota_r = lax.broadcasted_iota(jnp.int32, (BOXZ * XW, cols), 0)

    def step(i, c):
        for u in range(UNROLL):
            b = i * UNROLL + u
            (value,) = pick(1, b, corner_ref, offs_ref, img_ref, iota_y, iota_r)
            rows = jnp.broadcast_to(value, (16, cols)).astype(BF16)
            bend = lax.dot_general(rows, interp_ref[b], NT, preferred_element_type=F32)
            curv_ref[pl.ds(b, 1), :] = scale_ref[pl.ds(b, 1), :] * bend[0:1]
        return c

    lax.fori_loop(0, blocks // UNROLL, step, 0)


VM = pl.BlockSpec(memory_space=pltpu.VMEM)
SM = pl.BlockSpec(memory_space=pltpu.SMEM)


def neighbours(ring):
    chip = lax.axis_index(PTS[0])
    core = lax.axis_index(PTS[1])
    right = {PTS[0]: lax.rem(chip + 1, ring)}
    left = {PTS[0]: lax.rem(chip + ring - 1, ring)}
    mate = {PTS[1]: 1 - core}
    return chip, core, (right, left), mate


def greet(ways, mate):
    barrier = pltpu.get_barrier_semaphore()
    for other in (*ways, mate):
        pl.semaphore_signal(barrier, inc=1, device_id=other, device_id_type=MESH)
    pl.semaphore_wait(barrier, 3)


def gather_kernel(ring, x_ref, out_ref, buf, send_sem, recv_sem, mate_send, mate_recv, out_sem):
    chip, core, ways, mate = neighbours(ring)
    chunks = x_ref.shape[0]
    half = ring // 2
    own = chip * 2 + core

    def source(way, s):
        return lax.rem(chip + ring - 1 - s, ring) if way == 0 else lax.rem(chip + 1 + s, ring)

    def pass_on(way, s, slot, k, src):
        return pltpu.make_async_remote_copy(
            src_ref=src,
            dst_ref=buf.at[slot, k],
            send_sem=send_sem.at[way, s, k],
            recv_sem=recv_sem.at[way, s, k],
            device_id=ways[way],
            device_id_type=MESH,
        )

    def hand_over(index, slot, k, src):
        return pltpu.make_async_remote_copy(
            src_ref=src,
            dst_ref=buf.at[slot, k],
            send_sem=mate_send.at[index, k],
            recv_sem=mate_recv.at[index, k],
            device_id=mate,
            device_id_type=MESH,
        )

    greet(ways, mate)
    for k in range(chunks):
        for way in range(2):
            pass_on(way, 0, own, k, x_ref.at[k]).start()
    for k in range(chunks):
        hand_over(ring - 1, own, k, x_ref.at[k]).start()
    buf[own] = x_ref[...]

    def receive(way, s, k, forward):
        slot = source(way, s) * 2 + core
        here = buf.at[slot, k]
        pass_on(way, s, slot, k, here).wait_recv()
        if forward:
            pass_on(way, s + 1, slot, k, here).start()
        hand_over(way * half + s, slot, k, here).start()

    def step(s, c):
        for k in range(chunks):
            receive(0, s, k, True)
            receive(1, s, k, True)
        return c

    lax.fori_loop(0, half - 2, step, 0)
    for k in range(chunks):
        receive(0, half - 2, k, True)
        receive(1, half - 2, k, False)
    for k in range(chunks):
        receive(0, half - 1, k, False)

    def settle(way, s):
        slot = source(way, s) * 2 + core
        theirs = source(way, s) * 2 + 1 - core
        for k in range(chunks):
            pass_on(way, s, slot, k, buf.at[slot, k]).wait_send()
            hand_over(way * half + s, slot, k, buf.at[slot, k]).wait_send()
            hand_over(way * half + s, theirs, k, buf.at[theirs, k]).wait_recv()

    def settle_both(s, c):
        settle(0, s)
        settle(1, s)
        return c

    lax.fori_loop(0, half - 1, settle_both, 0)
    settle(0, half - 1)
    theirs = chip * 2 + 1 - core
    for k in range(chunks):
        hand_over(ring - 1, own, k, buf.at[own, k]).wait_send()
        hand_over(ring - 1, theirs, k, buf.at[theirs, k]).wait_recv()
    copy = pltpu.make_async_copy(buf, out_ref, out_sem)
    copy.start()
    copy.wait()


def ring_gather(block, call):
    ring = lax.axis_size(PTS[0])
    chunks = block.shape[0]
    return pl.pallas_call(
        functools.partial(gather_kernel, ring),
        name="ring_gather",
        in_specs=[VM],
        out_specs=pl.BlockSpec(memory_space=pl.ANY),
        out_shape=jax.ShapeDtypeStruct((2 * ring, *block.shape), block.dtype),
        scratch_shapes=[
            pltpu.VMEM((2 * ring, *block.shape), block.dtype),
            pltpu.SemaphoreType.DMA((2, ring // 2, chunks)),
            pltpu.SemaphoreType.DMA((2, ring // 2, chunks)),
            pltpu.SemaphoreType.DMA((ring, chunks)),
            pltpu.SemaphoreType.DMA((ring, chunks)),
            pltpu.SemaphoreType.DMA,
        ],
        compiler_params=pltpu.CompilerParams(
            collective_id=call, has_side_effects=True, vmem_limit_bytes=VMEM_CAP
        ),
    )(block)


def reduce_kernel(ring, x_ref, out_ref, mates, work, held, send_sem, recv_sem, mate_send, mate_recv):
    chip, core, ways, mate = neighbours(ring)
    chunks = x_ref.shape[2]
    half = ring // 2

    def target(way, s):
        return lax.rem(chip + half - s, ring) if way == 0 else lax.rem(chip + half + 1 + s, ring)

    def hand_over(index, t):
        return pltpu.make_async_remote_copy(
            src_ref=x_ref.at[t, 1 - core],
            dst_ref=mates.at[t],
            send_sem=mate_send.at[index],
            recv_sem=mate_recv.at[index],
            device_id=mate,
            device_id_type=MESH,
        )

    def pass_on(way, s, k):
        return pltpu.make_async_remote_copy(
            src_ref=work.at[way, s, k],
            dst_ref=held.at[way, s, k],
            send_sem=send_sem.at[way, s, k],
            recv_sem=recv_sem.at[way, s, k],
            device_id=ways[way],
            device_id_type=MESH,
        )

    greet(ways, mate)

    def give(s, c):
        hand_over(s, target(0, s)).start()
        hand_over(half + s, target(1, s)).start()
        return c

    lax.fori_loop(0, half - 1, give, 0)
    hand_over(half - 1, target(0, half - 1)).start()
    hand_over(ring - 1, chip).start()

    def local(t, k):
        return x_ref[t, core, k].astype(F32) + mates[t, k].astype(F32)

    def send(way, s, first):
        t = target(way, s)
        hand_over(way * half + s, t).wait_recv()
        for k in range(chunks):
            total = local(t, k)
            if not first:
                pass_on(way, s - 1, k).wait_recv()
                total = total + held[way, s - 1, k].astype(F32)
            work[way, s, k] = total.astype(BF16)
            pass_on(way, s, k).start()

    send(0, 0, True)
    send(1, 0, True)

    def step(s, c):
        send(0, s, False)
        send(1, s, False)
        return c

    lax.fori_loop(1, half - 1, step, 0)
    send(0, half - 1, False)
    hand_over(ring - 1, chip).wait_recv()
    for k in range(chunks):
        pass_on(1, half - 2, k).wait_recv()
        pass_on(0, half - 1, k).wait_recv()
        out_ref[k] = local(chip, k) + held[0, half - 1, k].astype(F32) + held[1, half - 2, k].astype(F32)

    def settle(way, s):
        hand_over(way * half + s, target(way, s)).wait_send()
        for k in range(chunks):
            pass_on(way, s, k).wait_send()

    def settle_both(s, c):
        settle(0, s)
        settle(1, s)
        return c

    lax.fori_loop(0, half - 1, settle_both, 0)
    settle(0, half - 1)
    hand_over(ring - 1, chip).wait_send()


def ring_reduce(blocks, call):
    ring, _, *inside = blocks.shape
    chunks = inside[0]
    return pl.pallas_call(
        functools.partial(reduce_kernel, ring),
        name="ring_reduce",
        in_specs=[VM],
        out_specs=VM,
        out_shape=jax.ShapeDtypeStruct(tuple(inside), F32),
        scratch_shapes=[
            pltpu.VMEM((ring, *inside), BF16),
            pltpu.VMEM((2, ring // 2, *inside), BF16),
            pltpu.VMEM((2, ring // 2, *inside), BF16),
            pltpu.SemaphoreType.DMA((2, ring // 2, chunks)),
            pltpu.SemaphoreType.DMA((2, ring // 2, chunks)),
            pltpu.SemaphoreType.DMA((ring,)),
            pltpu.SemaphoreType.DMA((ring,)),
        ],
        compiler_params=pltpu.CompilerParams(
            collective_id=call, has_side_effects=True, vmem_limit_bytes=VMEM_CAP
        ),
    )(blocks)


def split(values, count):
    terms = []
    for _ in range(count):
        high = lax.reduce_precision(values, 8, 7)
        terms.append(high.astype(BF16))
        values = values - high
    return terms


def split_pair(table):
    return jnp.concatenate(split(table, 2), axis=1)


def plane_of(fields, kern_y, kern_z):
    inner = jnp.einsum("fxbc,zc->fxbz", fields, kern_z, precision=HIGHEST)
    return jnp.einsum("fxbz,yb->xfzy", inner, kern_y, precision=HIGHEST).astype(BF16)


def body(
    grid_weights,
    direction,
    kern_x,
    kern_y,
    kern_z,
    interp,
    block_corner,
    block_offsets,
    labels,
    trial_steps,
    accept,
):
    slab, size_y, size_z = grid_weights.shape
    devices = lax.axis_size(PTS)
    size_x = slab * devices
    blocks, per_block, cols = interp.shape
    points = blocks * per_block * devices
    me = lax.axis_index(PTS)

    plane = plane_of(jnp.stack([grid_weights, direction]), kern_y, kern_z)
    gathered = ring_gather(plane.reshape(2 * slab, size_z, size_y), 0)
    gathered = gathered.reshape(size_x, 2, size_z, size_y)
    mine = lax.dynamic_slice_in_dim(kern_x, me * slab, slab, 0)
    tall = jnp.concatenate([kern_x, mine, mine, jnp.zeros((16 - 2 * slab, size_x), F32)], axis=0)
    kxs = split_pair(tall)
    own = jnp.concatenate([grid_weights, direction], axis=0).transpose(2, 0, 1)
    own = jnp.pad(own, ((0, 0), (0, 8 - 2 * slab), (0, 0)))
    stats, bend_scale, spread_all = pl.pallas_call(
        points_kernel,
        name="points",
        in_specs=[SM, SM, SM, VM, VM, VM, VM, VM, VM],
        out_specs=[VM, VM, VM],
        out_shape=[
            jax.ShapeDtypeStruct((16, 128), F32),
            jax.ShapeDtypeStruct((blocks, per_block), F32),
            jax.ShapeDtypeStruct((size_x, size_z, size_y), BF16),
        ],
        scratch_shapes=[
            pltpu.VMEM(((ZC + 1) * LINE, 128), F32),
            pltpu.VMEM(((ZC + 1) * LINE, 128), F32),
            pltpu.VMEM((2, size_z, size_x, size_y), BF16),
            pltpu.VMEM((blocks, per_block), F32),
            pltpu.VMEM((blocks, per_block), F32),
            pltpu.VMEM((blocks, per_block), F32),
            pltpu.VMEM(((size_z + 1) * LINE, 128), F32),
        ],
        compiler_params=pltpu.CompilerParams(vmem_limit_bytes=VMEM_CAP),
    )(block_corner, trial_steps, accept, gathered, kxs, own, block_offsets, interp, labels)

    chosen = jnp.sum(jnp.where(jnp.arange(NTRIAL) == accept[0], trial_steps, 0.0))
    new_weights = grid_weights + chosen * direction
    cores = lax.axis_size(PTS[1])
    spread = ring_reduce(spread_all.reshape(devices // cores, cores, slab, size_z, size_y), 1)
    grid_gradient = spread.transpose(0, 2, 1) - new_weights

    bend_plane = plane_of(grid_gradient[None], kern_y, kern_z)
    tail = jnp.pad(jnp.stack(split(jnp.sum(stats, axis=1), 3), axis=1), ((0, 0), (0, size_y - 3)))
    tail = jnp.stack([tail] + [jnp.zeros_like(tail)] * (slab - 1))[:, None]
    bend_block = jnp.concatenate([bend_plane, tail], axis=2).reshape(-1, (size_z + 16) * slab // 3, size_y)
    bend_gathered = ring_gather(bend_block, 2).reshape(size_x, 1, size_z + 16, size_y)
    tails = bend_gathered.reshape(devices, slab, size_z + 16, size_y)[:, 0, size_z:, :3]
    sums = jnp.sum(tails.astype(F32), axis=(0, 2))
    loglik = sums[:NTRIAL]
    descent = sums[NTRIAL : 2 * NTRIAL]
    quad_gu, quad_du, quad_dv = sums[10], sums[11], sums[12]
    prior = 0.5 * (quad_gu + 2.0 * trial_steps * quad_du + trial_steps * trial_steps * quad_dv)
    trial_objective = (loglik - prior) / points
    trial_slope = (descent - quad_du - trial_steps * quad_dv) / points

    curvature = pl.pallas_call(
        bend_kernel,
        name="bend",
        in_specs=[SM, VM, VM, VM, VM, VM],
        out_specs=VM,
        out_shape=jax.ShapeDtypeStruct((blocks, per_block), F32),
        scratch_shapes=[
            pltpu.VMEM(((ZC + 1) * LINE, 128), F32),
            pltpu.VMEM((1, size_z, size_x, size_y), BF16),
        ],
        compiler_params=pltpu.CompilerParams(vmem_limit_bytes=VMEM_CAP),
    )(block_corner, bend_gathered, split_pair(kern_x), block_offsets, interp, bend_scale)
    return (new_weights, grid_gradient, curvature, trial_objective, trial_slope)


def solution(mesh):
    cores = 2
    chips = mesh.shape["pts"] // cores
    finer = Mesh(mesh.devices.reshape(mesh.shape["parts"], chips, cores), PARTS_PTS)
    placed = (
        P(PARTS_PTS, None, None),
        P(PARTS_PTS, None, None),
        P(),
        P(),
        P(),
        P(PARTS_PTS, None, None),
        P(None, PARTS_PTS),
        P(PARTS_PTS, None),
        P(PARTS_PTS, None),
        P(),
        P(),
    )
    return jax.shard_map(
        body,
        mesh=finer,
        in_specs=placed,
        out_specs=(
            P(PARTS_PTS, None, None),
            P(PARTS_PTS, None, None),
            P(PARTS_PTS, None),
            P("parts"),
            P("parts"),
        ),
        check_vma=False,
    )
```
